32 devices in a mesh: group: 2 (over y), fsdp: 16 (over z, x, core).
Axes of the slice: x: 2, y: 2, z: 4, core: 2. Of those that a mesh axis runs over, the one named last changes fastest.
Arguments:
- teacher_rows: bfloat16 [20480, 2048], P(('group', 'fsdp')), may hold values from -6 to 6
- student_rows: bfloat16 [20480, 1024], P(('group', 'fsdp')), may hold values from -6 to 6
- counts: int32 [32], P(('group', 'fsdp')), may hold values from 213 to 640, as said below
- teacher_weight: bfloat16 [2048, 4096], P(None, ('group', 'fsdp')), may hold values from -0.125 to 0.125
- teacher_bias: float32 [4096], replicated, may hold values from -6 to 6
- teacher_gain: float32 [4096], replicated, may hold values from 0.1 to 1.9
- teacher_head: float32 [4096], replicated, may hold values from -0.09375 to 0.09375
- cross_weight: bfloat16 [1024, 1024], replicated, may hold values from -0.1875 to 0.1875
- cross_bias: float32 [1024], replicated, may hold values from -3 to 3
- out_weight: float32 [1024], replicated, may hold values from -0.1875 to 0.1875
Outputs:
- grad_cross: float32 [1024, 1024], P('fsdp')
- grad_bias: float32 [1024], replicated
- grad_out: float32 [1024], replicated
The draws below stay inside these ranges and needn't reach their ends.
Inputs may be any that keep to these rules, and one draw needn't show every extreme that they name: counts[i] live impressions fill the first slots of shard i, the rest of its 640 slots are padding.
All inputs are finite; a program needn't handle non-finite values.
Results may differ from the reference program's by a relative error of at most 0.00035.
The reference program's roundings to bfloat16 on the way (of `dcross_half`) count: a program that leaves them out, or rounds other values in their place, can miss the bound.
Values may be sent and summed in bfloat16 or wider, within the bound.
A program may use at most 128 MiB of HBM per device.

```python
import math
import jax
import jax.numpy as jnp
from jax import lax

FIN = 2048
DT = 4096
DS = 1024
ROWS_DEV = 640
SHARDS = 32
IMPR = 20480
N_GROUP = 2
N_FSDP = 16


def draw_counts(key, part):
    lowest = ROWS_DEV // 3
    spread = max(ROWS_DEV // 8, 1)
    position = jnp.arange(SHARDS, dtype=jnp.int32)
    trend = lowest + (ROWS_DEV - lowest) * position // max(SHARDS - 1, 1)
    jitter = jax.random.randint(key, (SHARDS,), -spread, spread + 1, dtype=jnp.int32)
    values = jnp.clip(trend + jitter, lowest, ROWS_DEV)
    values = values.at[0].set(lowest)
    values = values.at[SHARDS - 1].set(ROWS_DEV)
    return values.astype(jnp.int32)


def strengthened(array, stream_key, source, target, parts, factor):
    owner, partner = [(jnp.arange(array.shape[dim]) // (array.shape[dim] // parts)).reshape([-1 if axis == dim else 1 for axis in range(array.ndim)]) for dim in (source, target)]
    chosen = jax.random.permutation(stream_key, parts)[partner]
    strong = (owner == chosen) | (owner == (partner + parts // 2) % parts)
    return jnp.where(strong, factor * array, array)


def shard_levels(stream_key, extent, shards, smallest, largest):
    def one(axis_at, shards_of):
        steps = jax.random.uniform(jax.random.fold_in(jax.random.fold_in(stream_key, 6), axis_at), (shards_of,), jnp.float32, smallest / len(shards), largest / len(shards))
        return jnp.repeat(jnp.exp(steps), extent[axis_at] // shards_of).reshape((-1,) + (1,) * (len(extent) - axis_at - 1))

    level = one(*shards[0])
    for cut in shards[1:]:
        level = level * one(*cut)
    return level


def gaussian(stream_key, dims, deviation, most, split=(), held_as=jnp.bfloat16):
    values = jax.random.normal(stream_key, dims, jnp.float32) * deviation
    if len(split) > 0:
        values = shard_levels(stream_key, dims, split, -0.22, 0.18) * values
    return jnp.clip(values, min=-most, max=most).astype(held_as)


def heavy_noise(rng, extent, width, reach, cuts, heavy, kind=jnp.bfloat16):
    result = width * jax.random.normal(rng, extent, jnp.float32)
    if cuts:
        result = result * shard_levels(rng, extent, cuts, -0.22, 0.18)
    return jnp.clip(strengthened(result, jax.random.fold_in(rng, 3), *heavy), -reach, reach).astype(kind)


def setup_inputs(seed: int = 0) -> dict:
    keys = jax.random.split(jax.random.key(seed), 11)
    return {
        "teacher_rows": gaussian(keys[0], (IMPR, FIN), 1.0, 6.0, ((0, 32),)),
        "student_rows": heavy_noise(keys[1], (IMPR, DS), 1.0, 6.0, ((0, 32),), (0, 1, 32, 2.75)),
        "counts": draw_counts(jax.random.fold_in(keys[10], 71), 0),
        "teacher_weight": gaussian(keys[3], (FIN, DT), FIN ** -0.5, 0.125, ((1, 32),)),
        "teacher_bias": gaussian(keys[4], (DT,), 1.0, 6.0, (), jnp.float32),
        "teacher_gain": jnp.clip(1.0 + 0.18 * jax.random.normal(keys[5], (DT,), jnp.float32), 0.1, 1.9),
        "teacher_head": gaussian(keys[6], (DT,), DT ** -0.5, 0.09375, (), jnp.float32),
        "cross_weight": gaussian(keys[7], (DS, DS), DS ** -0.5, 0.1875),
        "cross_bias": gaussian(keys[8], (DS,), 0.5, 3.0, (), jnp.float32),
        "out_weight": gaussian(keys[9], (DS,), DS ** -0.5, 0.1875, (), jnp.float32),
    }


epsilon = 1e-06

def local_terms(rows_t, rows_s, amount, teacher_weight, teacher_bias, teacher_gain, teacher_head, cross_weight, cross_bias, out_weight, loss_scale):
    preact = jnp.dot(rows_t, teacher_weight, preferred_element_type=jnp.float32) + teacher_bias
    meansq = lax.optimization_barrier(jnp.mean(preact * preact, axis=-1, keepdims=True))
    normed = preact * lax.rsqrt(meansq + epsilon) * teacher_gain
    teacher_logit = lax.optimization_barrier(jnp.sum(jax.nn.silu(normed) * teacher_head, axis=-1))
    cross = jnp.dot(rows_s, cross_weight, preferred_element_type=jnp.float32) + cross_bias
    inputs_f = rows_s.astype(jnp.float32)
    mixed = inputs_f * cross + inputs_f
    student_logit = lax.optimization_barrier(jnp.sum(mixed * out_weight, axis=-1))
    live_rows = (jnp.arange(rows_t.shape[0], dtype=jnp.int32) < amount).astype(jnp.float32)
    error = (student_logit - teacher_logit) * live_rows * loss_scale
    dcross = error[:, None] * out_weight[None, :] * inputs_f
    dcross_half = dcross.astype(jnp.bfloat16)
    term_w = lax.dot_general(rows_s, dcross_half, (((0,), (0,)), ((), ())), preferred_element_type=jnp.float32)
    term_b = lax.optimization_barrier(jnp.sum(dcross, axis=0))
    term_o = lax.optimization_barrier(jnp.sum(error[:, None] * mixed, axis=0))
    return (term_w, term_b, term_o)

def reference(teacher_rows, student_rows, counts, teacher_weight, teacher_bias, teacher_gain, teacher_head, cross_weight, cross_bias, out_weight):
    shard_count = N_GROUP * N_FSDP
    loss_scale = math.sqrt(DS / (ROWS_DEV * shard_count))
    blocks_t = teacher_rows.reshape(shard_count, ROWS_DEV, FIN)
    blocks_s = student_rows.reshape(shard_count, ROWS_DEV, DS)

    def visit(carry, inputs):
        rows_t, rows_s, amount = inputs
        terms = local_terms(rows_t, rows_s, amount, teacher_weight, teacher_bias, teacher_gain, teacher_head, cross_weight, cross_bias, out_weight, loss_scale)
        return ((carry[0] + terms[0], carry[1] + terms[1], carry[2] + terms[2]), None)
    start_sums = (jnp.zeros((DS, DS), jnp.float32), jnp.zeros((DS,), jnp.float32), jnp.zeros((DS,), jnp.float32))
    totals, unused = lax.scan(visit, start_sums, (blocks_t, blocks_s, counts))
    return (totals[0], totals[1], totals[2])
```

```python
import functools
import math

import jax
import jax.numpy as jnp
from jax import lax
from jax.experimental import pallas as pl
from jax.experimental.pallas import tpu as pltpu
from jax.sharding import PartitionSpec as P

epsilon = 1e-06


def shards(
    teacher_rows,
    student_rows,
    counts,
    teacher_weight,
    teacher_bias,
    teacher_gain,
    teacher_head,
    cross_weight,
    cross_bias,
    out_weight,
):
    row_count = teacher_rows.shape[0]
    width_s = cross_weight.shape[0]
    group_count = lax.axis_size("group")
    fsdp_count = lax.axis_size("fsdp")
    shard_count = group_count * fsdp_count
    loss_scale = math.sqrt(width_s / (row_count * shard_count))
    preact = jnp.dot(
        teacher_rows,
        lax.all_gather(teacher_weight, ("group", "fsdp"), axis=1, tiled=True),
        preferred_element_type=jnp.float32,
    )
    preact = preact + teacher_bias
    meansq = jnp.mean(preact * preact, axis=-1, keepdims=True)
    normed = preact * lax.rsqrt(meansq + epsilon) * teacher_gain
    teacher_logit = jnp.sum(jax.nn.silu(normed) * teacher_head, axis=-1)
    cross = jnp.dot(student_rows, cross_weight, preferred_element_type=jnp.float32) + cross_bias
    inputs_f = student_rows.astype(jnp.float32)
    mixed = inputs_f * cross + inputs_f
    student_logit = jnp.sum(mixed * out_weight, axis=-1)
    live_rows = (jnp.arange(row_count, dtype=jnp.int32) < counts[0]).astype(jnp.float32)
    error = (student_logit - teacher_logit) * live_rows * loss_scale
    dcross = error[:, None] * out_weight[None, :] * inputs_f
    dcross_half = dcross.astype(jnp.bfloat16)
    term_b = jnp.sum(dcross, axis=0)
    term_o = jnp.sum(error[:, None] * mixed, axis=0)
    term_w = lax.dot_general(
        student_rows, dcross_half, (((0,), (0,)), ((), ())), preferred_element_type=jnp.float32
    )
    totals = lax.psum((term_w, term_b, term_o), "group")
    grad_cross = lax.psum_scatter(totals[0], "fsdp", scatter_dimension=0, tiled=True)
    small_sums = lax.psum((totals[1], totals[2]), "fsdp")
    return (grad_cross, small_sums[0], small_sums[1])


MESH = pl.DeviceIdType.MESH
LANES = 128
PAIRS = 2


def fused(fsdp_count, rp, t_ref, s_ref, live_ref, w_ref, bias_ref, gain_ref, head_ref, cw_ref, cb_ref, ow_ref,
          out_ref, small_ref,
          wbuf, rows, xs, cw, pre, ssq, gains, heads, mixed, msg1, in1, msg2, in2, rr, er, xt, dbuf,
          tw, r1, s1, r2, tt, r3, fin, r4, sb, rb, rz, lsem, ssem, rsem):
    g = lax.axis_index("group")
    f = lax.axis_index("fsdp")
    core = lax.rem(f, 2)
    x = lax.rem(lax.div(f, 2), 2)
    z = lax.div(f, 4)
    nz = fsdp_count // 4
    row_count, fin_width = t_ref.shape
    width_s = s_ref.shape[1]
    block = width_s // fsdp_count
    half_rows = block // 2
    rt = row_count // LANES
    units = bias_ref.shape[0] * LANES
    parts = 2 * PAIRS
    pw = width_s // parts

    def at(y_, z_, x_, c_):
        return (y_, (z_ * 2 + x_) * 2 + c_)

    partner = at(g, z, x, 1 - core)
    xn = at(g, z, 1 - x, core)
    yn = at(1 - g, z, x, core)
    barrier = pltpu.get_barrier_semaphore()
    peers = [partner, xn, yn] + [at(g, lax.rem(z + k, nz), x, core) for k in range(1, nz)]
    for peer in peers:
        pl.semaphore_signal(barrier, inc=1, device_id=peer, device_id_type=MESH)

    locals_ = []
    for i, (a, b) in enumerate([
        (s_ref, xs.at[pl.ds(0, row_count)]),
        (cw_ref, cw),
        (w_ref, wbuf.at[0]),
        (t_ref, rows.at[pl.ds(0, row_count)]),
    ]):
        cp = pltpu.make_async_copy(a, b, lsem.at[i])
        cp.start()
        locals_.append(cp)
    pl.semaphore_wait(barrier, len(peers))

    sends = []

    def send(a, b, device):
        i = len(sends)
        cp = pltpu.make_async_remote_copy(
            src_ref=a, dst_ref=b, send_sem=ssem.at[i], recv_sem=rsem.at[i], device_id=device, device_id_type=MESH
        )
        cp.start()
        sends.append(cp)
        return cp

    def slot(dx, dy, dz):
        return (dx * 2 + dy) * nz + dz

    order = [1] + list(range(nz - 1, 1, -1))
    xin, yin, zin, din = {}, {}, {}, {}
    xin[0] = send(w_ref, wbuf.at[slot(1, 0, 0)], xn)
    yin[0] = send(w_ref, wbuf.at[slot(0, 1, 0)], yn)
    for k in order:
        zin[k] = send(w_ref, wbuf.at[slot(0, 0, k)], at(g, lax.rem(z + nz - k, nz), x, core))
    rows_in = send(t_ref, rows.at[pl.ds(row_count, row_count)], partner)
    xs_in = send(s_ref, xs.at[pl.ds(row_count, row_count)], partner)

    depth = fin_width // 2

    def forward(k):
        xin[k].wait_recv()
        a = send(wbuf.at[slot(1, 0, k), pl.ds(0, depth)], wbuf.at[slot(1, 1, k), pl.ds(0, depth)], yn)
        yin[k].wait_recv()
        b = send(wbuf.at[slot(0, 1, k), pl.ds(depth, depth)], wbuf.at[slot(1, 1, k), pl.ds(depth, depth)], xn)
        din[k] = (a, b)

    def relay(k):
        zin[k].wait_recv()
        xin[k] = send(wbuf.at[slot(0, 0, k)], wbuf.at[slot(1, 0, k)], xn)
        yin[k] = send(wbuf.at[slot(0, 0, k)], wbuf.at[slot(0, 1, k)], yn)

    eye = lax.broadcasted_iota(jnp.int32, (LANES, LANES), 0) == lax.broadcasted_iota(jnp.int32, (LANES, LANES), 1)

    def to_row(col):
        return jnp.sum(jnp.where(eye, col, 0.0), axis=0, keepdims=True)

    def to_col(row):
        return jnp.sum(jnp.where(eye, row, 0.0), axis=1, keepdims=True)

    def tile(t):
        return pl.ds(pl.multiple_of(t * LANES, LANES), LANES)

    ssq[...] = jnp.zeros_like(ssq)
    for ref in (msg1, msg2, er, rr):
        ref[...] = jnp.zeros_like(ref)
    msg1[pl.ds(3 * rp, rt), :] = live_ref[...]

    locals_[0].wait()
    locals_[1].wait()
    ow = ow_ref[...]

    def student(t, carry):
        xt_ = xs[tile(t), :]
        cross = jnp.dot(xt_, cw[...], preferred_element_type=jnp.float32) + cb_ref[...]
        xf = xt_.astype(jnp.float32)
        m = xf * cross + xf
        mixed[tile(t), :] = m
        msg1[pl.ds(2 * rp + t, 1), :] = to_row(jnp.sum(m * ow, axis=1, keepdims=True))
        return carry

    lax.fori_loop(0, rt, student, 0)
    locals_[2].wait()
    locals_[3].wait()

    mt = 2 * LANES

    def project(dx, dy, dz):
        s = slot(dx, dy, dz)
        y_ = g if dy == 0 else 1 - g
        x_ = x if dx == 0 else 1 - x
        index = y_ * fsdp_count + (lax.rem(z + dz, nz) * 2 + x_) * 2 + core
        gains[pl.ds(s, 1), :] = gain_ref[index] * 0.5
        heads[pl.ds(s, 1), :] = head_ref[index]
        bias = bias_ref[index]

        def step(t, carry):
            ds = pl.ds(pl.multiple_of(t * mt, mt), mt)
            p = jnp.dot(rows[ds, :], wbuf[s], preferred_element_type=jnp.float32) + bias
            pre[s, ds, :] = p
            ssq[ds, :] += p * p
            return carry

        lax.fori_loop(0, 2 * row_count // mt, step, 0)

    forward(0)
    rows_in.wait_recv()
    project(0, 0, 0)
    relay(order[0])
    project(1, 0, 0)
    project(0, 1, 0)

    xs_in.wait_recv()
    pick = (
        lax.broadcasted_iota(jnp.int32, (block, 2 * block), 1)
        == lax.broadcasted_iota(jnp.int32, (block, 2 * block), 0) + core * block
    )
    pick = jnp.where(pick, 1.0, 0.0).astype(jnp.bfloat16)
    for j in range(fsdp_count // 2):
        xt[pl.ds(j * block, block), :] = lax.dot_general(
            pick, xs[:, pl.ds(j * 2 * block, 2 * block)], (((1,), (1,)), ((), ())), preferred_element_type=jnp.float32
        ).astype(jnp.bfloat16)

    previous = 0
    for n, k in enumerate(order):
        if n > 0:
            relay(k)
        project(0, 0, k)
        for cp in din[previous]:
            cp.wait_recv()
        project(1, 1, previous)
        forward(k)
        project(1, 0, k)
        project(0, 1, k)
        previous = k
    for cp in din[previous]:
        cp.wait_recv()
    project(1, 1, previous)

    for h in range(2):
        def squares(t, carry, h=h):
            col = jnp.sum(ssq[tile(h * rt + t), :], axis=1, keepdims=True)
            msg1[pl.ds(h * rp + t, 1), :] = to_row(col)
            return carry

        lax.fori_loop(0, rt, squares, 0)
    m1 = send(msg1, in1, partner)
    m1.wait_recv()
    for h in range(2):
        total = msg1[pl.ds(h * rp, rp), :] + in1[pl.ds((1 - h) * rp, rp), :]
        rr[pl.ds(h * rp, rp), :] = lax.rsqrt(total * (1.0 / units) + epsilon)

    for h in range(2):
        def logits(t, carry, h=h):
            r = to_col(rr[pl.ds(h * rp + t, 1), :])
            acc = jnp.zeros((LANES, LANES), jnp.float32)
            for s in range(4 * nz):
                v = pre[s, tile(h * rt + t), :] * r * gains[pl.ds(s, 1), :]
                acc += (v * jnp.tanh(v) + v) * heads[pl.ds(s, 1), :]
            msg2[pl.ds(h * rp + t, 1), :] = to_row(jnp.sum(acc, axis=1, keepdims=True))
            return carry

        lax.fori_loop(0, rt, logits, 0)
    m2 = send(msg2, in2, partner)
    m2.wait_recv()
    for h, src in ((0, msg1), (1, in1)):
        teacher = msg2[pl.ds(h * rp, rp), :] + in2[pl.ds((1 - h) * rp, rp), :]
        er[pl.ds(h * rp, rp), :] = (src[pl.ds(2 * rp, rp), :] - teacher) * src[pl.ds(3 * rp, rp), :]

    sb[...] = jnp.zeros_like(sb)

    def own(t, carry):
        e = to_col(er[pl.ds(t, 1), :])
        d = e * ow * xs[tile(t), :].astype(jnp.float32)
        dbuf[tile(t), :] = d.astype(jnp.bfloat16)
        sb[0, pl.ds(0, 1), :] += jnp.sum(d, axis=0, keepdims=True)
        sb[0, pl.ds(1, 1), :] += jnp.sum(e * mixed[tile(t), :], axis=0, keepdims=True)
        return carry

    lax.fori_loop(0, rt, own, 0)
    c0 = send(sb.at[0], rb.at[0], partner)

    def other(t, carry):
        e = to_col(er[pl.ds(rp + t, 1), :])
        d = e * ow * xs[tile(rt + t), :].astype(jnp.float32)
        dbuf[tile(rt + t), :] = d.astype(jnp.bfloat16)
        return carry

    lax.fori_loop(0, rt, other, 0)

    def way(p):
        return (g, x, yn, xn) if p % 2 == 0 else (x, g, xn, yn)

    h1, h2, h3, h4 = {}, {}, {}, {}
    for p in range(parts):
        val = jnp.dot(xt[...], dbuf[:, pl.ds(p * pw, pw)], preferred_element_type=jnp.float32)
        for z_ in range(nz):
            for x_ in range(2):
                for y_ in range(2):
                    first, second = (y_, x_) if p % 2 == 0 else (x_, y_)
                    offset = ((z_ * 2 + x_) * 2 + y_) * half_rows
                    tw[p, first, second, z_] = val[offset:offset + half_rows, :]
        first, second, n1, n2 = way(p)
        h1[p] = send(tw.at[p, 1 - first], r1.at[p], n1)
    c0.wait_recv()
    sb[1] = sb[0] + rb[0]
    c1 = send(sb.at[1], rb.at[1], xn)

    def stage2(p):
        first, second, n1, n2 = way(p)
        h1[p].wait_recv()
        s1[p] = tw[p, first] + r1[p]
        h2[p] = send(s1.at[p, 1 - second], r2.at[p], n2)

    def stage3(p):
        first, second, n1, n2 = way(p)
        h2[p].wait_recv()
        tt[p] = s1[p, second] + r2[p]
        h3[p] = []
        for k in range(1, nz):
            to = lax.rem(z + k, nz)
            h3[p].append(send(tt.at[p, to], r3.at[p, k - 1], at(g, to, x, core)))

    def stage4(p):
        total = tt[p, z]
        for k in range(nz - 1):
            h3[p][k].wait_recv()
            total = total + r3[p, k]
        fin[p] = total
        h4[p] = send(fin.at[p], r4.at[p], yn)
        out_ref[pl.ds(pl.multiple_of(g * half_rows, half_rows), half_rows), pl.ds(p * pw, pw)] = total

    for p in range(parts):
        stage2(p)
        if p == 1:
            c1.wait_recv()
            sb[2] = sb[1] + rb[1]
            c2 = send(sb.at[2], rb.at[2], yn)
    for p in range(parts):
        stage3(p)
        if p == 1:
            c2.wait_recv()
            sb[3] = sb[2] + rb[2]
            rz[z] = sb[3]
            cz = []
            for k in range(1, nz):
                to = lax.rem(z + k, nz)
                cz.append(send(sb.at[3], rz.at[z], at(g, to, x, core)))
    for p in range(parts):
        stage4(p)
    for cp in cz:
        cp.wait_recv()
    total = rz[0]
    for k in range(1, nz):
        total = total + rz[k]
    small_ref[...] = total
    for p in range(parts):
        h4[p].wait_recv()
        out_ref[pl.ds(pl.multiple_of((1 - g) * half_rows, half_rows), half_rows), pl.ds(p * pw, pw)] = r4[p]
    for cp in sends:
        cp.wait_send()


def shards_fused(
    teacher_rows,
    student_rows,
    counts,
    teacher_weight,
    teacher_bias,
    teacher_gain,
    teacher_head,
    cross_weight,
    cross_bias,
    out_weight,
):
    row_count, fin_width = teacher_rows.shape
    width_s = cross_weight.shape[0]
    group_count = lax.axis_size("group")
    fsdp_count = lax.axis_size("fsdp")
    loss_scale = math.sqrt(width_s / (row_count * group_count * fsdp_count))
    live = (jnp.arange(row_count, dtype=jnp.int32) < counts[0]).astype(jnp.float32) * loss_scale
    rt = row_count // LANES
    rp = -(-rt // 8) * 8
    nz = fsdp_count // 4
    block = width_s // fsdp_count
    half_rows = block // 2
    parts = 2 * PAIRS
    pw = width_s // parts
    slots = 4 * nz
    f32, bf16 = jnp.float32, jnp.bfloat16
    vm = pltpu.VMEM
    split = lambda v: v.reshape(-1, 1, LANES)
    anyspec = pl.BlockSpec(memory_space=pl.ANY)
    vspec = pl.BlockSpec(memory_space=pltpu.VMEM)
    grad, small = pl.pallas_call(
        functools.partial(fused, fsdp_count, rp),
        out_shape=(jax.ShapeDtypeStruct((block, width_s), f32), jax.ShapeDtypeStruct((8, width_s), f32)),
        in_specs=[anyspec, anyspec, vspec, anyspec, vspec, vspec, vspec, anyspec, vspec, vspec],
        out_specs=(vspec, vspec),
        scratch_shapes=[
            vm((slots, fin_width, LANES), bf16),
            vm((2 * row_count, fin_width), bf16),
            vm((2 * row_count, width_s), bf16),
            vm((width_s, width_s), bf16),
            vm((slots, 2 * row_count, LANES), f32),
            vm((2 * row_count, LANES), f32),
            vm((slots, LANES), f32),
            vm((slots, LANES), f32),
            vm((row_count, width_s), f32),
            vm((4 * rp, LANES), f32),
            vm((4 * rp, LANES), f32),
            vm((2 * rp, LANES), f32),
            vm((2 * rp, LANES), f32),
            vm((2 * rp, LANES), f32),
            vm((2 * rp, LANES), f32),
            vm((width_s // 2, 2 * row_count), bf16),
            vm((2 * row_count, width_s), bf16),
            vm((parts, 2, 2, nz, half_rows, pw), f32),
            vm((parts, 2, nz, half_rows, pw), f32),
            vm((parts, 2, nz, half_rows, pw), f32),
            vm((parts, nz, half_rows, pw), f32),
            vm((parts, nz, half_rows, pw), f32),
            vm((parts, nz - 1, half_rows, pw), f32),
            vm((parts, half_rows, pw), f32),
            vm((parts, half_rows, pw), f32),
            vm((4, 8, width_s), f32),
            vm((3, 8, width_s), f32),
            vm((nz, 8, width_s), f32),
            pltpu.SemaphoreType.DMA((4,)),
            pltpu.SemaphoreType.DMA((SEMS,)),
            pltpu.SemaphoreType.DMA((SEMS,)),
        ],
        compiler_params=pltpu.CompilerParams(
            collective_id=0, has_side_effects=True, vmem_limit_bytes=60 * 1024 * 1024
        ),
    )(
        teacher_rows, student_rows, live.reshape(rt, LANES), teacher_weight, split(teacher_bias), split(teacher_gain),
        split(teacher_head), cross_weight, cross_bias[None, :], out_weight[None, :],
    )
    return (grad, small[0], small[1])


SEMS = 64


def fits(mesh, args):
    rows, fin_width = args[0].shape
    width_s = args[1].shape[1]
    units = args[3].shape[1]
    group_count, fsdp_count = mesh.shape["group"], mesh.shape["fsdp"]
    devices = group_count * fsdp_count
    return (
        group_count == 2
        and fsdp_count % 4 == 0
        and fsdp_count >= 8
        and fsdp_count <= 16
        and units == devices * LANES
        and (rows // devices) % LANES == 0
        and (2 * width_s // fsdp_count) % LANES == 0
        and width_s % (2 * PAIRS * LANES) == 0
    )


def solution(mesh):
    in_specs = (
        P(("group", "fsdp"), None),
        P(("group", "fsdp"), None),
        P(("group", "fsdp")),
        P(None, ("group", "fsdp")),
        P(),
        P(),
        P(),
        P(),
        P(),
        P(),
    )
    out_specs = (P("fsdp", None), P(), P())

    def run(*args):
        body = shards_fused if fits(mesh, args) else shards
        return jax.shard_map(body, mesh=mesh, in_specs=in_specs, out_specs=out_specs, check_vma=False)(*args)

    return run
```

```python
import functools
import math

import jax
import jax.numpy as jnp
from jax import lax
from jax.experimental import pallas as pl
from jax.experimental.pallas import tpu as pltpu
from jax.sharding import PartitionSpec as P

epsilon = 1e-06


def shards(
    teacher_rows,
    student_rows,
    counts,
    teacher_weight,
    teacher_bias,
    teacher_gain,
    teacher_head,
    cross_weight,
    cross_bias,
    out_weight,
):
    row_count = teacher_rows.shape[0]
    width_s = cross_weight.shape[0]
    group_count = lax.axis_size("group")
    fsdp_count = lax.axis_size("fsdp")
    shard_count = group_count * fsdp_count
    loss_scale = math.sqrt(width_s / (row_count * shard_count))
    preact = jnp.dot(
        teacher_rows,
        lax.all_gather(teacher_weight, ("group", "fsdp"), axis=1, tiled=True),
        preferred_element_type=jnp.float32,
    )
    preact = preact + teacher_bias
    meansq = jnp.mean(preact * preact, axis=-1, keepdims=True)
    normed = preact * lax.rsqrt(meansq + epsilon) * teacher_gain
    teacher_logit = jnp.sum(jax.nn.silu(normed) * teacher_head, axis=-1)
    cross = jnp.dot(student_rows, cross_weight, preferred_element_type=jnp.float32) + cross_bias
    inputs_f = student_rows.astype(jnp.float32)
    mixed = inputs_f * cross + inputs_f
    student_logit = jnp.sum(mixed * out_weight, axis=-1)
    live_rows = (jnp.arange(row_count, dtype=jnp.int32) < counts[0]).astype(jnp.float32)
    error = (student_logit - teacher_logit) * live_rows * loss_scale
    dcross = error[:, None] * out_weight[None, :] * inputs_f
    dcross_half = dcross.astype(jnp.bfloat16)
    term_b = jnp.sum(dcross, axis=0)
    term_o = jnp.sum(error[:, None] * mixed, axis=0)
    term_w = lax.dot_general(
        student_rows, dcross_half, (((0,), (0,)), ((), ())), preferred_element_type=jnp.float32
    )
    totals = lax.psum((term_w, term_b, term_o), "group")
    grad_cross = lax.psum_scatter(totals[0], "fsdp", scatter_dimension=0, tiled=True)
    small_sums = lax.psum((totals[1], totals[2]), "fsdp")
    return (grad_cross, small_sums[0], small_sums[1])


MESH = pl.DeviceIdType.MESH
LANES = 128
PAIRS = 4


def fused(fsdp_count, rp, t_ref, s_ref, live_ref, w_ref, bias_ref, gain_ref, head_ref, cw_ref, cb_ref, ow_ref,
          out_ref, small_ref,
          wbuf, rows, xs, cw, pre, ssq, gains, heads, mixed, msg1, in1, msg2, in2, rr, er, xt, dbuf,
          tw, r1, s1, r2, tt, r3, fin, r4, sb, rb, rz, lsem, ssem, rsem):
    g = lax.axis_index("group")
    f = lax.axis_index("fsdp")
    core = lax.rem(f, 2)
    x = lax.rem(lax.div(f, 2), 2)
    z = lax.div(f, 4)
    nz = fsdp_count // 4
    row_count, fin_width = t_ref.shape
    width_s = s_ref.shape[1]
    block = width_s // fsdp_count
    half_rows = block // 2
    rt = row_count // LANES
    units = bias_ref.shape[0] * LANES
    parts = 2 * PAIRS
    pw = width_s // parts

    def at(y_, z_, x_, c_):
        return (y_, (z_ * 2 + x_) * 2 + c_)

    partner = at(g, z, x, 1 - core)
    xn = at(g, z, 1 - x, core)
    yn = at(1 - g, z, x, core)
    barrier = pltpu.get_barrier_semaphore()
    peers = [partner, xn, yn] + [at(g, lax.rem(z + k, nz), x, core) for k in range(1, nz)]
    for peer in peers:
        pl.semaphore_signal(barrier, inc=1, device_id=peer, device_id_type=MESH)

    locals_ = []
    for i, (a, b) in enumerate([
        (s_ref, xs.at[pl.ds(0, row_count)]),
        (cw_ref, cw),
        (w_ref, wbuf.at[0]),
        (t_ref, rows.at[pl.ds(0, row_count)]),
    ]):
        cp = pltpu.make_async_copy(a, b, lsem.at[i])
        cp.start()
        locals_.append(cp)
    pl.semaphore_wait(barrier, len(peers))

    sends = []

    def send(a, b, device):
        i = len(sends)
        cp = pltpu.make_async_remote_copy(
            src_ref=a, dst_ref=b, send_sem=ssem.at[i], recv_sem=rsem.at[i], device_id=device, device_id_type=MESH
        )
        cp.start()
        sends.append(cp)
        return cp

    def slot(dx, dy, dz):
        return (dx * 2 + dy) * nz + dz

    order = [1] + list(range(nz - 1, 1, -1))
    depth = fin_width // 2
    xin, yin, zin, din = {}, {}, {}, {}

    def half(ref, h):
        return ref.at[pl.ds(h * depth, depth)]

    def piece(dx, dy, dz, h):
        return wbuf.at[slot(dx, dy, dz), pl.ds(h * depth, depth)]

    def zpeer(k):
        return at(g, lax.rem(z + nz - k, nz), x, core)

    for h in range(2):
        xin[0, h] = send(half(w_ref, h), piece(1, 0, 0, h), xn)
        yin[0, h] = send(half(w_ref, h), piece(0, 1, 0, h), yn)
        zin[order[0], h] = send(half(w_ref, h), piece(0, 0, order[0], h), zpeer(order[0]))
    for k in order[1:]:
        for h in range(2):
            zin[k, h] = send(half(w_ref, h), piece(0, 0, k, h), zpeer(k))
    rows_in = send(t_ref, rows.at[pl.ds(row_count, row_count)], partner)
    xs_in = send(s_ref, xs.at[pl.ds(row_count, row_count)], partner)

    def diagonal(k, h):
        lo, hi = pl.ds(h * depth, depth // 2), pl.ds(h * depth + depth // 2, depth // 2)
        xin[k, h].wait_recv()
        a = send(wbuf.at[slot(1, 0, k), lo], wbuf.at[slot(1, 1, k), lo], yn)
        yin[k, h].wait_recv()
        b = send(wbuf.at[slot(0, 1, k), hi], wbuf.at[slot(1, 1, k), hi], xn)
        din[k, h] = (a, b)

    def relay(k, h):
        zin[k, h].wait_recv()
        xin[k, h] = send(piece(0, 0, k, h), piece(1, 0, k, h), xn)
        yin[k, h] = send(piece(0, 0, k, h), piece(0, 1, k, h), yn)

    def arrived(k, h):
        for cp in din[k, h]:
            cp.wait_recv()

    def along(k, h):
        arrived(0, h)
        din[k, h] = (send(piece(1, 1, 0, h), piece(1, 1, k, h), zpeer(k)),)

    eye = lax.broadcasted_iota(jnp.int32, (LANES, LANES), 0) == lax.broadcasted_iota(jnp.int32, (LANES, LANES), 1)

    def to_row(col):
        return jnp.sum(jnp.where(eye, col, 0.0), axis=0, keepdims=True)

    def to_col(row):
        return jnp.sum(jnp.where(eye, row, 0.0), axis=1, keepdims=True)

    def tile(t):
        return pl.ds(pl.multiple_of(t * LANES, LANES), LANES)

    ssq[...] = jnp.zeros_like(ssq)
    for ref in (msg1, msg2, er, rr):
        ref[...] = jnp.zeros_like(ref)
    msg1[pl.ds(3 * rp, rt), :] = live_ref[...]

    locals_[0].wait()
    locals_[1].wait()
    ow = ow_ref[...]

    def student(t, carry):
        xt_ = xs[tile(t), :]
        cross = jnp.dot(xt_, cw[...], preferred_element_type=jnp.float32) + cb_ref[...]
        xf = xt_.astype(jnp.float32)
        m = xf * cross + xf
        mixed[tile(t), :] = m
        msg1[pl.ds(2 * rp + t, 1), :] = to_row(jnp.sum(m * ow, axis=1, keepdims=True))
        return carry

    lax.fori_loop(0, rt, student, 0)
    locals_[2].wait()
    locals_[3].wait()

    mt = row_count

    def project(dx, dy, dz):
        s = slot(dx, dy, dz)
        y_ = g if dy == 0 else 1 - g
        x_ = x if dx == 0 else 1 - x
        index = y_ * fsdp_count + (lax.rem(z + dz, nz) * 2 + x_) * 2 + core
        gains[pl.ds(s, 1), :] = gain_ref[index] * 0.5
        heads[pl.ds(s, 1), :] = head_ref[index]
        bias = bias_ref[index]

        def step(t, carry):
            ds = pl.ds(pl.multiple_of(t * mt, mt), mt)
            p = jnp.dot(rows[ds, :], wbuf[s], preferred_element_type=jnp.float32) + bias
            pre[s, ds, :] = p
            ssq[ds, :] += p * p
            return carry

        lax.fori_loop(0, 2 * row_count // mt, step, 0)

    lead = order[0]
    for h in range(2):
        diagonal(0, h)
        relay(lead, h)
    rows_in.wait_recv()
    project(0, 0, 0)
    along(lead, 0)
    project(1, 0, 0)
    project(0, 1, 0)

    xs_in.wait_recv()
    pick = (
        lax.broadcasted_iota(jnp.int32, (block, 2 * block), 1)
        == lax.broadcasted_iota(jnp.int32, (block, 2 * block), 0) + core * block
    )
    pick = jnp.where(pick, 1.0, 0.0).astype(jnp.bfloat16)
    for j in range(fsdp_count // 2):
        xt[pl.ds(j * block, block), :] = lax.dot_general(
            pick, xs[:, pl.ds(j * 2 * block, 2 * block)], (((1,), (1,)), ((), ())), preferred_element_type=jnp.float32
        ).astype(jnp.bfloat16)

    along(lead, 1)
    ready = [(1, 1, 0), (0, 0, lead)]
    late = []
    before = None
    for k in order[1:]:
        if before is not None:
            diagonal(before, 0)
        relay(k, 0)
        if before is not None:
            diagonal(before, 1)
            ready += [(1, 0, before), (0, 1, before)]
        else:
            for h in range(2):
                xin[lead, h].wait_recv()
                yin[lead, h].wait_recv()
            late += [(1, 0, lead), (0, 1, lead)]
        for item in ready:
            project(*item)
        relay(k, 1)
        ready = late + [(0, 0, k)]
        late = []
        before = k
    diagonal(before, 0)
    for item in ready:
        project(*item)
    for k in order[1:-1]:
        for h in range(2):
            arrived(k, h)
        project(1, 1, k)
    diagonal(before, 1)
    project(1, 0, before)
    project(0, 1, before)
    for k in (lead, before):
        for h in range(2):
            arrived(k, h)
        project(1, 1, k)

    for h in range(2):
        def squares(t, carry, h=h):
            col = jnp.sum(ssq[tile(h * rt + t), :], axis=1, keepdims=True)
            msg1[pl.ds(h * rp + t, 1), :] = to_row(col)
            return carry

        lax.fori_loop(0, rt, squares, 0)
    m1 = send(msg1, in1, partner)
    m1.wait_recv()
    for h in range(2):
        total = msg1[pl.ds(h * rp, rp), :] + in1[pl.ds((1 - h) * rp, rp), :]
        rr[pl.ds(h * rp, rp), :] = lax.rsqrt(total * (1.0 / units) + epsilon)

    for h in range(2):
        def logits(t, carry, h=h):
            r = to_col(rr[pl.ds(h * rp + t, 1), :])
            acc = jnp.zeros((LANES, LANES), jnp.float32)
            for s in range(4 * nz):
                v = pre[s, tile(h * rt + t), :] * r * gains[pl.ds(s, 1), :]
                acc += (v * jnp.tanh(v) + v) * heads[pl.ds(s, 1), :]
            msg2[pl.ds(h * rp + t, 1), :] = to_row(jnp.sum(acc, axis=1, keepdims=True))
            return carry

        lax.fori_loop(0, rt, logits, 0)
    m2 = send(msg2, in2, partner)
    m2.wait_recv()
    for h, src in ((0, msg1), (1, in1)):
        teacher = msg2[pl.ds(h * rp, rp), :] + in2[pl.ds((1 - h) * rp, rp), :]
        er[pl.ds(h * rp, rp), :] = (src[pl.ds(2 * rp, rp), :] - teacher) * src[pl.ds(3 * rp, rp), :]

    sb[...] = jnp.zeros_like(sb)

    def own(t, carry):
        e = to_col(er[pl.ds(t, 1), :])
        d = e * ow * xs[tile(t), :].astype(jnp.float32)
        dbuf[tile(t), :] = d.astype(jnp.bfloat16)
        sb[0, pl.ds(0, 1), :] += jnp.sum(d, axis=0, keepdims=True)
        sb[0, pl.ds(1, 1), :] += jnp.sum(e * mixed[tile(t), :], axis=0, keepdims=True)
        return carry

    lax.fori_loop(0, rt, own, 0)
    c0 = send(sb.at[0], rb.at[0], partner)

    def other(t, carry):
        e = to_col(er[pl.ds(rp + t, 1), :])
        d = e * ow * xs[tile(rt + t), :].astype(jnp.float32)
        dbuf[tile(rt + t), :] = d.astype(jnp.bfloat16)
        return carry

    lax.fori_loop(0, rt, other, 0)

    def way(p):
        return (g, x, yn, xn) if p % 2 == 0 else (x, g, xn, yn)

    h1, h2, h3, h4 = {}, {}, {}, {}

    def stage1(p):
        val = jnp.dot(xt[...], dbuf[:, pl.ds(p * pw, pw)], preferred_element_type=jnp.float32)
        for z_ in range(nz):
            for x_ in range(2):
                for y_ in range(2):
                    first, second = (y_, x_) if p % 2 == 0 else (x_, y_)
                    offset = ((z_ * 2 + x_) * 2 + y_) * half_rows
                    tw[p, first, second, z_] = val[offset:offset + half_rows, :]
        first, second, n1, n2 = way(p)
        h1[p] = send(tw.at[p, 1 - first], r1.at[p], n1)

    def stage2(p):
        first, second, n1, n2 = way(p)
        h1[p].wait_recv()
        s1[p] = tw[p, first] + r1[p]
        h2[p] = send(s1.at[p, 1 - second], r2.at[p], n2)

    def stage3(p):
        first, second, n1, n2 = way(p)
        h2[p].wait_recv()
        tt[p] = s1[p, second] + r2[p]
        h3[p] = []
        for k in range(1, nz):
            to = lax.rem(z + k, nz)
            h3[p].append(send(tt.at[p, to], r3.at[p, k - 1], at(g, to, x, core)))

    def stage4(p):
        total = tt[p, z]
        for k in range(nz - 1):
            h3[p][k].wait_recv()
            total = total + r3[p, k]
        fin[p] = total
        h4[p] = send(fin.at[p], r4.at[p], yn)
        out_ref[pl.ds(pl.multiple_of(g * half_rows, half_rows), half_rows), pl.ds(p * pw, pw)] = total

    cz = []

    def small(n):
        if n == 0:
            c0.wait_recv()
            sb[1] = sb[0] + rb[0]
            cz.append(send(sb.at[1], rb.at[1], xn))
        elif n == 1:
            cz.pop().wait_recv()
            sb[2] = sb[1] + rb[1]
            cz.append(send(sb.at[2], rb.at[2], yn))
        elif n == 2:
            cz.pop().wait_recv()
            sb[3] = sb[2] + rb[2]
            rz[z] = sb[3]
            for k in range(1, nz):
                to = lax.rem(z + k, nz)
                cz.append(send(sb.at[3], rz.at[z], at(g, to, x, core)))

    stages = (stage1, stage2, stage3, stage4)
    lag = (0, 2, 3, 5)
    for step in range(PAIRS + lag[-1]):
        for stage, behind in zip(stages, lag):
            q = step - behind
            if 0 <= q < PAIRS:
                stage(2 * q)
                stage(2 * q + 1)
        small(step - 1)
    for cp in cz:
        cp.wait_recv()
    total = rz[0]
    for k in range(1, nz):
        total = total + rz[k]
    small_ref[...] = total
    for p in range(parts):
        h4[p].wait_recv()
        out_ref[pl.ds(pl.multiple_of((1 - g) * half_rows, half_rows), half_rows), pl.ds(p * pw, pw)] = r4[p]
    for cp in sends:
        cp.wait_send()


def shards_fused(
    teacher_rows,
    student_rows,
    counts,
    teacher_weight,
    teacher_bias,
    teacher_gain,
    teacher_head,
    cross_weight,
    cross_bias,
    out_weight,
):
    row_count, fin_width = teacher_rows.shape
    width_s = cross_weight.shape[0]
    group_count = lax.axis_size("group")
    fsdp_count = lax.axis_size("fsdp")
    loss_scale = math.sqrt(width_s / (row_count * group_count * fsdp_count))
    live = (jnp.arange(row_count, dtype=jnp.int32) < counts[0]).astype(jnp.float32) * loss_scale
    rt = row_count // LANES
    rp = -(-rt // 8) * 8
    nz = fsdp_count // 4
    block = width_s // fsdp_count
    half_rows = block // 2
    parts = 2 * PAIRS
    pw = width_s // parts
    slots = 4 * nz
    f32, bf16 = jnp.float32, jnp.bfloat16
    vm = pltpu.VMEM
    split = lambda v: v.reshape(-1, 1, LANES)
    anyspec = pl.BlockSpec(memory_space=pl.ANY)
    vspec = pl.BlockSpec(memory_space=pltpu.VMEM)
    grad, small = pl.pallas_call(
        functools.partial(fused, fsdp_count, rp),
        out_shape=(jax.ShapeDtypeStruct((block, width_s), f32), jax.ShapeDtypeStruct((8, width_s), f32)),
        in_specs=[anyspec, anyspec, vspec, anyspec, vspec, vspec, vspec, anyspec, vspec, vspec],
        out_specs=(vspec, vspec),
        scratch_shapes=[
            vm((slots, fin_width, LANES), bf16),
            vm((2 * row_count, fin_width), bf16),
            vm((2 * row_count, width_s), bf16),
            vm((width_s, width_s), bf16),
            vm((slots, 2 * row_count, LANES), f32),
            vm((2 * row_count, LANES), f32),
            vm((slots, LANES), f32),
            vm((slots, LANES), f32),
            vm((row_count, width_s), f32),
            vm((4 * rp, LANES), f32),
            vm((4 * rp, LANES), f32),
            vm((2 * rp, LANES), f32),
            vm((2 * rp, LANES), f32),
            vm((2 * rp, LANES), f32),
            vm((2 * rp, LANES), f32),
            vm((width_s // 2, 2 * row_count), bf16),
            vm((2 * row_count, width_s), bf16),
            vm((parts, 2, 2, nz, half_rows, pw), f32),
            vm((parts, 2, nz, half_rows, pw), f32),
            vm((parts, 2, nz, half_rows, pw), f32),
            vm((parts, nz, half_rows, pw), f32),
            vm((parts, nz, half_rows, pw), f32),
            vm((parts, nz - 1, half_rows, pw), f32),
            vm((parts, half_rows, pw), f32),
            vm((parts, half_rows, pw), f32),
            vm((4, 8, width_s), f32),
            vm((3, 8, width_s), f32),
            vm((nz, 8, width_s), f32),
            pltpu.SemaphoreType.DMA((4,)),
            pltpu.SemaphoreType.DMA((SEMS,)),
            pltpu.SemaphoreType.DMA((SEMS,)),
        ],
        compiler_params=pltpu.CompilerParams(
            collective_id=0, has_side_effects=True, vmem_limit_bytes=60 * 1024 * 1024
        ),
    )(
        teacher_rows, student_rows, live.reshape(rt, LANES), teacher_weight, split(teacher_bias), split(teacher_gain),
        split(teacher_head), cross_weight, cross_bias[None, :], out_weight[None, :],
    )
    return (grad, small[0], small[1])


SEMS = 112


def fits(mesh, args):
    rows, fin_width = args[0].shape
    width_s = args[1].shape[1]
    units = args[3].shape[1]
    group_count, fsdp_count = mesh.shape["group"], mesh.shape["fsdp"]
    devices = group_count * fsdp_count
    return (
        group_count == 2
        and fsdp_count % 4 == 0
        and fsdp_count >= 8
        and fsdp_count <= 16
        and units == devices * LANES
        and (rows // devices) % LANES == 0
        and (2 * width_s // fsdp_count) % LANES == 0
        and width_s % (2 * PAIRS * LANES) == 0
    )


def solution(mesh):
    in_specs = (
        P(("group", "fsdp"), None),
        P(("group", "fsdp"), None),
        P(("group", "fsdp")),
        P(None, ("group", "fsdp")),
        P(),
        P(),
        P(),
        P(),
        P(),
        P(),
    )
    out_specs = (P("fsdp", None), P(), P())

    def run(*args):
        body = shards_fused if fits(mesh, args) else shards
        return jax.shard_map(body, mesh=mesh, in_specs=in_specs, out_specs=out_specs, check_vma=False)(*args)

    return run
```
